256 devices in a mesh: gx: 4 (over x), gy: 8 (over y, core), gz: 8 (over z).
Axes of the slice: x: 4, y: 4, z: 8, core: 2. Of those that a mesh axis runs over, the one named last changes fastest.
Arguments:
- dual_operators: bfloat16 [4, 8, 8, 768, 768], P('gx', 'gy', 'gz'), may hold values from -1 to 3, as said below
- dual_load: float32 [4, 8, 8, 32, 384], P('gx', 'gy', 'gz'), may hold values from -25 to 25
- rigid_modes: float32 [4, 8, 8, 6, 768], P('gx', 'gy', 'gz'), may hold values from -0.21875 to 0.21875
- coarse_load: float32 [4, 8, 8, 6, 32], P('gx', 'gy', 'gz'), may hold values from -24 to 24
- mode_counts: int32 [4, 8, 8], P('gx', 'gy', 'gz'), may hold values from 3 to 6
- face_maps: int32 [4, 8, 8, 3, 128], P('gx', 'gy', 'gz'), may hold values from 0 to 127, each once within a row
Outputs:
- multipliers: float32 [4, 8, 8, 32, 384], P('gx', 'gy', 'gz')
- residual: float32 [4, 8, 8, 32, 384], P('gx', 'gy', 'gz')
The draws below stay inside these ranges and needn't reach their ends.
Inputs may be any that keep to these rules, and one draw needn't show every extreme that they name: Each dual_operators[i, j, k] is symmetric positive definite. Subdomain s uses rows 0 to mode_counts[s] - 1 of rigid_modes[s]. Each face_maps[i, j, k, d] holds every number of 0 to 127 once.
All inputs are finite; a program needn't handle non-finite values.
Results may differ from the reference program's by a relative error of at most 0.012.
Values sent between devices are 32-bit elements; how exact they have to be, the bound alone decides.
No kernel may reach another device: no remote copies, remote signals or barrier semaphores. Data moves between devices by JAX's collectives and lax.ppermute only.
A program may use at most 64 MiB of HBM per device.

```python
import math
import jax
import jax.numpy as jnp
from jax import lax

IDOF = 768
FACE = 128
RHS = 32
MODES = 6
ITERS = 2
NSX = 4
NSY = 8
NSZ = 8


def draw_dual_operators(key, part):
    spread = 0.7 / math.sqrt(2.0 * IDOF)
    identity = jnp.eye(IDOF, dtype=jnp.float32)

    def one_column(position):
        column_key = jax.random.fold_in(key, position)
        noise_key = jax.random.fold_in(column_key, 1)
        scale_key = jax.random.fold_in(column_key, 2)
        noise_part = jax.random.truncated_normal(noise_key, -4.0, 4.0, (NSZ, IDOF, IDOF), jnp.float32) * spread
        coupling = identity + 0.5 * (noise_part + jnp.swapaxes(noise_part, 1, 2))
        diagonal = jnp.exp(jax.random.uniform(scale_key, (NSZ, IDOF), jnp.float32, math.log(0.25), math.log(2.0)))
        root_scale = jnp.sqrt(diagonal)
        outer_scale = root_scale[:, :, None] * root_scale[:, None, :]
        return (coupling * outer_scale).astype(jnp.bfloat16)
    blocks = lax.map(one_column, jnp.arange(NSX * NSY))
    return blocks.reshape(NSX, NSY, NSZ, IDOF, IDOF)


def draw_dual_load(key, part):
    grid_key = jax.random.fold_in(key, 11)
    column_key = jax.random.fold_in(key, 12)
    value_key = jax.random.fold_in(key, 13)
    location = (jnp.arange(NSX)[:, None, None] + jnp.arange(NSY)[None, :, None] + jnp.arange(NSZ)[None, None, :]).astype(jnp.float32) / (NSX + NSY + NSZ - 3)
    rising = (1.0 + 2.0 * location) / math.sqrt(3.0)
    subdomain_scale = jnp.exp(jax.random.uniform(grid_key, (NSX, NSY, NSZ), jnp.float32, math.log(0.1), math.log(1.0)))
    column_scale = jnp.exp(jax.random.uniform(column_key, (RHS,), jnp.float32, math.log(0.3), math.log(3.0)))
    full_shape = (NSX, NSY, NSZ, RHS, 3 * FACE)
    values = jax.random.truncated_normal(value_key, -4.0, 4.0, full_shape, jnp.float32)
    scales = (rising * subdomain_scale)[:, :, :, None, None] * column_scale[None, None, None, :, None]
    return values * scales


def set_ends(drawn, own_key, low, high):
    shape = drawn.shape
    index_at = [jax.random.randint(jax.random.fold_in(own_key, axis), (), 0, shape[axis]) for axis in range(len(shape))]
    drawn = drawn.at[tuple(index_at)].set(low)
    longest = shape.index(max(shape))
    index_at[longest] = (index_at[longest] + 1) % shape[longest]
    return drawn.at[tuple(index_at)].set(high)


def shard_levels(own_key, dims, split, smallest, largest):
    gain = 1.0
    for dim, shards_of in split:
        heights = jax.random.uniform(jax.random.fold_in(jax.random.fold_in(own_key, 6), dim), (shards_of,), jnp.float32, smallest / len(split), largest / len(split))
        gain = gain * jnp.repeat(jnp.exp(heights), dims[dim] // shards_of).reshape((-1,) + (1,) * (len(dims) - 1 - dim))
    return gain


def gaussian(own_key, dims, width, bound, cuts=(), kind=jnp.bfloat16):
    loudness = shard_levels(own_key, dims, cuts, -0.22, 0.18) if cuts else 1.0
    array = jax.random.normal(own_key, dims, jnp.float32) * width * loudness
    return jnp.minimum(jnp.maximum(array, -bound), bound).astype(kind)


def setup_inputs(seed: int = 0) -> dict:
    arg_keys = jax.random.split(jax.random.key(seed), 7)
    dual_operators = draw_dual_operators(jax.random.fold_in(arg_keys[6], 71), 0)
    dual_load = draw_dual_load(jax.random.fold_in(arg_keys[6], 71), 0)
    rigid_modes = gaussian(arg_keys[2], (NSX, NSY, NSZ, MODES, IDOF), IDOF ** -0.5, 0.21875, ((0, 4), (1, 8), (2, 8)), jnp.float32)
    coarse_load = gaussian(arg_keys[3], (NSX, NSY, NSZ, MODES, RHS), 4.0, 24.0, ((0, 4), (1, 8), (2, 8)), jnp.float32)
    mode_counts = set_ends(jax.random.randint(arg_keys[4], (NSX, NSY, NSZ), 3, MODES + 1), jax.random.fold_in(arg_keys[4], 1), 3, MODES).astype(jnp.int32)
    face_maps = jax.vmap(lambda own: jax.random.permutation(own, FACE))(jax.random.split(arg_keys[5], NSX * NSY * NSZ * 3)).reshape((NSX, NSY, NSZ, 3, FACE)).astype(jnp.int32)
    return dict(dual_operators=dual_operators, dual_load=dual_load, rigid_modes=rigid_modes, coarse_load=coarse_load, mode_counts=mode_counts, face_maps=face_maps)


def reorder(values, face_order):
    index_table = jnp.broadcast_to(face_order[..., None, :], values.shape)
    return jnp.take_along_axis(values, index_table, axis=-1)

def side_flags(position, extent):
    return jnp.stack([position > 0, position < extent - 1], axis=-1).astype(jnp.float32)

def interface_mask(first_flags, second_flags, third_flags, face_width):
    grid_shape = (first_flags.shape[0], second_flags.shape[0], third_flags.shape[0], 2)
    present = jnp.concatenate([jnp.broadcast_to(first_flags[:, None, None, :], grid_shape), jnp.broadcast_to(second_flags[None, :, None, :], grid_shape), jnp.broadcast_to(third_flags[None, None, :, :], grid_shape)], axis=-1)
    return jnp.repeat(present, face_width, axis=-1)[:, :, :, None, :]

def face_block(values, face_index, face_width):
    return values[..., face_index * face_width:(face_index + 1) * face_width]

def from_lower(block, spatial):
    length = block.shape[spatial]
    padding = jnp.zeros_like(lax.slice_in_dim(block, 0, 1, axis=spatial))
    return jnp.concatenate([padding, lax.slice_in_dim(block, 0, length - 1, axis=spatial)], axis=spatial)

def from_upper(block, spatial):
    length = block.shape[spatial]
    padding = jnp.zeros_like(lax.slice_in_dim(block, 0, 1, axis=spatial))
    return jnp.concatenate([lax.slice_in_dim(block, 1, length, axis=spatial), padding], axis=spatial)

def assemble(local_values, face_maps, inverse, present):
    pieces = []
    for spatial in range(3):
        minus_face = face_block(local_values, 2 * spatial, FACE)
        plus_face = face_block(local_values, 2 * spatial + 1, FACE)
        owner_minus = reorder(minus_face, inverse[:, :, :, spatial, :])
        pieces.append(minus_face - reorder(from_lower(plus_face, spatial), face_maps[:, :, :, spatial, :]))
        pieces.append(plus_face - from_upper(owner_minus, spatial))
    return jnp.concatenate(pieces, axis=-1) * present

def apply_dual(local_values, dual_operators, face_maps, inverse, present):
    rounded = local_values.astype(jnp.bfloat16)

    def one_slab(operands):
        slab_operators, slab_values = operands
        return jnp.einsum('yzrk,yzki->yzri', slab_values.astype(jnp.float32), slab_operators.astype(jnp.float32), precision=lax.Precision.HIGHEST)
    products = lax.map(one_slab, (dual_operators, rounded))
    return assemble(products, face_maps, inverse, present)

def coarse_factor(mode_rows, active):
    identity = jnp.eye(active.shape[-1], dtype=jnp.float32)
    normal_matrix = jnp.einsum('xyzmi,xyzni->xyzmn', mode_rows, mode_rows, precision=lax.Precision.HIGHEST)
    normal_matrix = normal_matrix + identity * (1.0 - active)[..., None, :]
    factor = jnp.linalg.cholesky(normal_matrix)
    return jax.scipy.linalg.cho_solve((factor, True), jnp.broadcast_to(identity, normal_matrix.shape))

def spread_coarse(coefficients, mode_rows):
    return jnp.einsum('xyzmr,xyzmi->xyzri', coefficients, mode_rows, precision=lax.Precision.HIGHEST)

def owned_faces(values):
    return jnp.concatenate([face_block(values, 1, FACE), face_block(values, 3, FACE), face_block(values, 5, FACE)], axis=-1)

def pairing(first_vectors, second_vectors):
    return jnp.einsum('xyzri,xyzsi->rs', owned_faces(first_vectors), owned_faces(second_vectors), precision=lax.Precision.HIGHEST)

def combine_columns(vectors, matrix):
    return jnp.einsum('xyzri,rs->xyzsi', vectors, matrix, precision=lax.Precision.HIGHEST)

def cholesky_solve(matrix, right_side):
    factor = jnp.linalg.cholesky(matrix)
    return jax.scipy.linalg.cho_solve((factor, True), right_side)

def reference(dual_operators, dual_load, rigid_modes, coarse_load, mode_counts, face_maps):
    present = interface_mask(side_flags(jnp.arange(NSX), NSX), side_flags(jnp.arange(NSY), NSY), side_flags(jnp.arange(NSZ), NSZ), FACE)
    inverse = jnp.argsort(face_maps, axis=-1).astype(jnp.int32)
    active = (jnp.arange(MODES)[None, None, None, :] < mode_counts[..., None]).astype(jnp.float32)
    mode_rows = rigid_modes * present * active[..., None]
    coarse_inverse = coarse_factor(mode_rows, active)

    def coarse_field(coefficients):
        return assemble(spread_coarse(coefficients, mode_rows), face_maps, inverse, present)

    def precondition(current):
        weights = jnp.einsum('xyzmi,xyzri->xyzmr', mode_rows, current, precision=lax.Precision.HIGHEST)
        coefficients = jnp.einsum('xyzmn,xyznr->xyzmr', coarse_inverse, weights, precision=lax.Precision.HIGHEST)
        return current - 0.25 * coarse_field(coefficients)

    def operator(current):
        return apply_dual(current, dual_operators, face_maps, inverse, present)
    empty_face = jnp.zeros_like(dual_load[..., :FACE])
    spread_load = jnp.concatenate([empty_face, dual_load[..., :FACE], empty_face, dual_load[..., FACE:2 * FACE], empty_face, dual_load[..., 2 * FACE:]], axis=-1)
    right_local = assemble(spread_load, face_maps, inverse, present)
    initial = coarse_field(jnp.einsum('xyzmn,xyznr->xyzmr', coarse_inverse, coarse_load * active[..., None], precision=lax.Precision.HIGHEST))
    multipliers = initial
    residual = right_local - operator(initial)
    direction = residual
    image = residual
    residual_gram = jnp.zeros((RHS, RHS), jnp.float32)
    for iteration in range(ITERS):
        projected = precondition(residual)
        projected_image = operator(projected)
        fresh_gram = pairing(projected, residual)
        if iteration == 0:
            direction = projected
            image = projected_image
        else:
            update_gram = cholesky_solve(residual_gram, fresh_gram)
            direction = projected + combine_columns(direction, update_gram)
            image = projected_image + combine_columns(image, update_gram)
        residual_gram = fresh_gram
        step_gram = cholesky_solve(pairing(direction, image), residual_gram)
        multipliers = multipliers + combine_columns(direction, step_gram)
        residual = residual - combine_columns(image, step_gram)
    return (owned_faces(multipliers), owned_faces(residual))
```

```python
import functools

import jax
import jax.numpy as jnp
import numpy as np
from jax import lax
from jax.experimental import pallas as pl
from jax.experimental.pallas import tpu as pltpu
from jax.sharding import Mesh
from jax.sharding import PartitionSpec as P


AXES = ("gx", "gy_0", "gy_1", "gz")
GY = ("gy_0", "gy_1")
HIGHEST = lax.Precision.HIGHEST
F32 = jnp.float32
BF16 = jnp.bfloat16


def involution(dims, partner):
    pairs = []
    for place in np.ndindex(*dims):
        pairs.append(
            (int(np.ravel_multi_index(place, dims)), int(np.ravel_multi_index(partner(*place), dims)))
        )
    back = dict(pairs)
    assert all(back[b] == a for a, b in pairs)
    return pairs


def shifted(i, n):
    return (i + 1) % n if i % 2 else (i - 1) % n


def matchings(dims):
    nx, ny, _, nz = dims
    halves = nz // 2

    def far_z(z):
        return (3 - z) % nz if z in (0, 3, 4, 7) and z < halves else (11 - z if z in (4, 7) else 7 - z)

    return {
        "x1": involution(dims, lambda x, y, c, z: (x ^ 1, y, c, z)),
        "x2": involution(dims, lambda x, y, c, z: (shifted(x, nx), y, c, z)),
        "y1": involution(dims, lambda x, y, c, z: (x, y, 1 - c, z)),
        "y2": involution(dims, lambda x, y, c, z: (x, (y + (1 if c else -1)) % ny, 1 - c, z)),
        "y3": involution(dims, lambda x, y, c, z: (x, (y + (-1 if c else 1)) % ny, 1 - c, z)),
        "z1": involution(dims, lambda x, y, c, z: (x, y, c, z ^ 1)),
        "z2": involution(dims, lambda x, y, c, z: (x, y, c, shifted(z, nz))),
        "z3": involution(dims, lambda x, y, c, z: (x, y, c, far_z(z))),
    }


HALO = ("x1", "x2", "y1", "y2", "z1", "z2")


def swap(array, pairs):
    return lax.ppermute(array, AXES, pairs)


def places():
    x = lax.axis_index("gx")
    core = lax.axis_index("gy_1")
    y = lax.axis_index("gy_0") * 2 + core
    z = lax.axis_index("gz")
    return (
        (x, lax.axis_size("gx")),
        (y, lax.axis_size("gy_0") * lax.axis_size("gy_1")),
        (z, lax.axis_size("gz")),
    )


def permuter(maps_ref, d):
    width = maps_ref.shape[-1]
    rows = lax.broadcasted_iota(jnp.int32, (width, width), 0)
    return jnp.where(rows == maps_ref[d : d + 1, :], 1.0, 0.0).astype(BF16)


def in_three(values):
    first = values.astype(BF16)
    rest = values - first.astype(F32)
    second = rest.astype(BF16)
    third = (rest - second.astype(F32)).astype(BF16)
    return jnp.concatenate([first, second, third], axis=0)


def reordered(values, one_hot, back):
    rows = values.shape[0]
    dims = (((1,), (1,)), ((), ())) if back else (((1,), (0,)), ((), ()))
    parts = lax.dot_general(in_three(values), one_hot, dims, preferred_element_type=F32)
    return parts[:rows] + parts[rows : 2 * rows] + parts[2 * rows :]


def write_sends(vector_of, maps_ref, send_refs):
    for d, (position, _) in enumerate(places()):
        odd = lax.rem(position, 2) == 1
        minus = vector_of(2 * d)
        plus = vector_of(2 * d + 1)
        owner_minus = reordered(minus, permuter(maps_ref, d), True)
        send_refs[2 * d][...] = jnp.where(odd, owner_minus, plus)
        send_refs[2 * d + 1][...] = jnp.where(odd, plus, owner_minus)


def difference(vector_ref, receive_refs, maps_ref):
    width = maps_ref.shape[-1]
    blocks = []
    for d, (position, extent) in enumerate(places()):
        odd = lax.rem(position, 2) == 1
        first = receive_refs[2 * d][...]
        second = receive_refs[2 * d + 1][...]
        below = jnp.where(odd, first, second)
        above = jnp.where(odd, second, first)
        minus = vector_ref[:, 2 * d * width : (2 * d + 1) * width]
        plus = vector_ref[:, (2 * d + 1) * width : (2 * d + 2) * width]
        lower = minus - reordered(below, permuter(maps_ref, d), False)
        blocks.append(jnp.where(position > 0, lower, 0.0))
        blocks.append(jnp.where(position < extent - 1, plus - above, 0.0))
    return blocks


def times_operator(values, operator_ref):
    rows = values.shape[0]
    high = values.astype(BF16)
    low = (values - high.astype(F32)).astype(BF16)
    both = jnp.dot(
        jnp.concatenate([high, low], axis=0), operator_ref[...], preferred_element_type=F32
    )
    return both[:rows] + both[rows:]


def dot_rows(first, second):
    return lax.dot_general(
        first, second, (((1,), (1,)), ((), ())), precision=HIGHEST, preferred_element_type=F32
    )


def dot_columns(first, second):
    return lax.dot_general(
        first, second, (((0,), (0,)), ((), ())), precision=HIGHEST, preferred_element_type=F32
    )


def dot(first, second):
    return jnp.dot(first, second, precision=HIGHEST, preferred_element_type=F32)


def coarse(values, modes_ref, dual_modes_ref):
    return dot(dot_rows(values, dual_modes_ref[...]), modes_ref[...])


def blocks_of(array, width):
    return lambda i: array[:, i * width : (i + 1) * width]


def eliminate(matrix, others, count):
    rows = matrix.shape[0]
    row_number = lax.broadcasted_iota(jnp.int32, (rows, 1), 0)
    for k in range(count):
        pivot = 1.0 / matrix[k : k + 1, k : k + 1]
        column = matrix[:, k : k + 1]
        reduced = []
        for part in (matrix, *others):
            row = part[k : k + 1, :] * pivot
            reduced.append(jnp.where(row_number == k, row, part - column * row))
        matrix, *others = reduced
    return others


def start_kernel(counts_ref, modes_in_ref, load_ref, maps_ref, modes_ref, dual_ref, vector_ref, *send_refs):
    width = maps_ref.shape[-1]
    count = counts_ref[0]
    total, size = modes_in_ref.shape
    rows = modes_ref.shape[0]
    modes_ref[...] = jnp.zeros_like(modes_ref)
    lane = lax.broadcasted_iota(jnp.int32, (total, width), 0)
    for d, (position, extent) in enumerate(places()):
        for side, there in ((0, position > 0), (1, position < extent - 1)):
            part = pl.ds((2 * d + side) * width, width)
            keep = jnp.logical_and(lane < count, there)
            modes_ref[0:total, part] = jnp.where(keep, modes_in_ref[:, part], 0.0)
    modes = modes_ref[...]
    one = lax.broadcasted_iota(jnp.int32, (rows, rows), 0)
    two = lax.broadcasted_iota(jnp.int32, (rows, rows), 1)
    normal = dot_rows(modes, modes) + jnp.where(jnp.logical_and(one == two, one >= count), 1.0, 0.0)
    row = lax.broadcasted_iota(jnp.int32, load_ref.shape, 0)
    dual_ref[...] = jnp.zeros_like(dual_ref)
    dual_ref[0:total, 0 : load_ref.shape[1]] = jnp.where(row < count, load_ref[...], 0.0)
    loads = dual_ref[:, 0 : load_ref.shape[1]]
    dual, coefficients = eliminate(normal, [modes, loads], total)
    dual_ref[...] = dual
    vector = dot_columns(coefficients, modes)
    vector_ref[...] = vector
    write_sends(blocks_of(vector, width), maps_ref, send_refs)


def first_kernel(operator_ref, load_ref, vector_ref, maps_ref, *refs):
    receive_refs, (lambda_ref, next_ref), send_refs = refs[:6], refs[6:8], refs[8:]
    width = maps_ref.shape[-1]
    blocks = difference(vector_ref, receive_refs, maps_ref)
    for d in range(3):
        lambda_ref[:, d * width : (d + 1) * width] = blocks[2 * d + 1]
    product = times_operator(jnp.concatenate(blocks, axis=1), operator_ref)
    parts = []
    for i in range(6):
        part = product[:, i * width : (i + 1) * width]
        parts.append(load_ref[:, (i // 2) * width : (i // 2 + 1) * width] - part if i % 2 else -part)
        next_ref[:, i * width : (i + 1) * width] = parts[i]
    write_sends(lambda i: parts[i], maps_ref, send_refs)


def coarse_kernel(modes_ref, dual_ref, vector_ref, maps_ref, *refs):
    receive_refs, (whole_ref, next_ref), send_refs = refs[:6], refs[6:8], refs[8:]
    width = maps_ref.shape[-1]
    whole = jnp.concatenate(difference(vector_ref, receive_refs, maps_ref), axis=1)
    whole_ref[...] = whole
    following = coarse(whole, modes_ref, dual_ref)
    next_ref[...] = following
    write_sends(blocks_of(following, width), maps_ref, send_refs)


def operator_kernel(operator_ref, base_ref, before_ref, vector_ref, maps_ref, *refs):
    receive_refs, (whole_ref, next_ref, gram_ref), send_refs = refs[:6], refs[6:9], refs[9:]
    width = maps_ref.shape[-1]
    whole = base_ref[...] - 0.25 * jnp.concatenate(
        difference(vector_ref, receive_refs, maps_ref), axis=1
    )
    whole_ref[...] = whole
    product = times_operator(whole, operator_ref)
    next_ref[...] = product
    write_sends(blocks_of(product, width), maps_ref, send_refs)
    gram_ref[...] = dot_rows(whole, jnp.concatenate([before_ref[...], product], axis=0))


def last_kernel(operator_ref, base_ref, before_ref, vector_ref, gram_in_ref, maps_ref, *refs):
    receive_refs, (whole_ref, next_ref, gram_ref), send_refs = refs[:6], refs[6:9], refs[9:]
    width = maps_ref.shape[-1]
    whole = base_ref[...] - 0.25 * jnp.concatenate(
        difference(vector_ref, receive_refs, maps_ref), axis=1
    )
    whole_ref[...] = whole
    product = times_operator(whole, operator_ref)
    next_ref[...] = product
    half = gram_in_ref.shape[1]
    gram_ref[:, 0:half] = gram_in_ref[...]
    gram_ref[:, half:] = dot_rows(whole, jnp.concatenate([before_ref[...], product], axis=0))
    for d in range(3):
        minus = product[:, 2 * d * width : (2 * d + 1) * width]
        send_refs[d][...] = reordered(minus, permuter(maps_ref, d), True)


def finish_kernel(
    gram_ref, lambda_ref, first_ref, second_ref, residual_ref, image_ref, product_ref, *refs
):
    receive_refs, (multipliers_ref, out_ref) = refs[:6], refs[6:]
    count = gram_ref.shape[0]
    width = product_ref.shape[1] // 6
    total = gram_ref[...]
    right = total[:, 0:count]
    energy, cross, last = (total[:, i * count : (i + 1) * count] for i in (1, 2, 3))
    energy = 0.5 * (energy + energy.T)
    last = 0.5 * (last + last.T)
    matrix = jnp.concatenate(
        [
            jnp.concatenate([energy, cross.T, right], axis=1),
            jnp.concatenate([cross, last, energy], axis=1),
        ],
        axis=0,
    )
    rows = 2 * count
    row_number = lax.broadcasted_iota(jnp.int32, (rows, 1), 0)
    for k in range(rows):
        row = matrix[k : k + 1, :] / matrix[k : k + 1, k : k + 1]
        matrix = jnp.where(row_number == k, row, matrix - matrix[:, k : k + 1] * row)
    step = matrix[0:count, rows : rows + count]
    other = matrix[count:rows, rows : rows + count]
    for d, (position, extent) in enumerate(places()):
        odd = lax.rem(position, 2) == 1
        above = jnp.where(odd, receive_refs[2 * d + 1][...], receive_refs[2 * d][...])
        at = slice((2 * d + 1) * width, (2 * d + 2) * width)
        to = slice(d * width, (d + 1) * width)
        second_image = jnp.where(position < extent - 1, product_ref[:, at] - above, 0.0)
        multipliers_ref[:, to] = (
            lambda_ref[:, to] + dot_columns(step, first_ref[:, at]) + dot_columns(other, second_ref[:, at])
        )
        out_ref[:, to] = (
            residual_ref[:, at] - dot_columns(step, image_ref[:, at]) - dot_columns(other, second_image)
        )


def call(kernel, shapes, *operands, smem=()):
    specs = [
        pl.BlockSpec(memory_space=pltpu.SMEM if i in smem else pltpu.VMEM) for i in range(len(operands))
    ]
    return pl.pallas_call(
        kernel,
        out_shape=[jax.ShapeDtypeStruct(s, F32) for s in shapes],
        in_specs=specs,
        out_specs=[pl.BlockSpec(memory_space=pltpu.VMEM)] * len(shapes),
        compiler_params=pltpu.CompilerParams(vmem_limit_bytes=16 * 2**20),
        name=kernel.__name__,
    )(*operands)


def local(pairs, dual_operators, dual_load, rigid_modes, coarse_load, mode_counts, face_maps):
    operator = dual_operators[0, 0, 0]
    load = dual_load[0, 0, 0]
    modes_in = rigid_modes[0, 0, 0]
    coefficients = coarse_load[0, 0, 0]
    counts = mode_counts.reshape(1)
    maps = face_maps[0, 0, 0]
    cases = load.shape[0]
    size = operator.shape[0]
    width = maps.shape[1]
    full, face = (cases, size), (cases, width)
    padded = (-(-modes_in.shape[0] // 8) * 8, size)

    def halo(sends):
        return [swap(send, pairs[name]) for send, name in zip(sends, HALO, strict=True)]

    modes, dual, vector, *sends = call(
        start_kernel, [padded, padded, full, *[face] * 6], counts, modes_in, coefficients, maps, smem=(0,)
    )
    initial, load_vector, *sends = call(
        first_kernel, [load.shape, full, *[face] * 6], operator, load, vector, maps, *halo(sends)
    )
    residual, vector, *sends = call(
        coarse_kernel, [full, full, *[face] * 6], modes, dual, load_vector, maps, *halo(sends)
    )
    first, product, gram, *sends = call(
        operator_kernel,
        [full, full, (cases, 2 * cases), *[face] * 6],
        operator,
        residual,
        load_vector,
        vector,
        maps,
        *halo(sends),
    )
    image, vector, *sends = call(
        coarse_kernel, [full, full, *[face] * 6], modes, dual, product, maps, *halo(sends)
    )
    second, product, gram, *sends = call(
        last_kernel,
        [full, full, (cases, 4 * cases), *[face] * 3],
        operator,
        image,
        product,
        vector,
        gram,
        maps,
        *halo(sends),
    )
    receives = {}
    for name in ("y1", "y2", "y3", "x1", "x2", "z1", "z2", "z3"):
        if name in HALO:
            mine = jnp.concatenate([sends["xyz".index(name[0])], gram], axis=0)
            theirs = swap(mine, pairs[name])
            receives[name] = theirs[:cases]
            gram = gram + theirs[cases:]
        else:
            gram = gram + swap(gram, pairs[name])
    multipliers, out = call(
        finish_kernel,
        [load.shape, load.shape],
        gram,
        initial,
        first,
        second,
        residual,
        image,
        product,
        *[receives[name] for name in HALO],
    )
    return multipliers[None, None, None], out[None, None, None]


def solution(mesh):
    dims = (mesh.shape["gx"], mesh.shape["gy"] // 2, 2, mesh.shape["gz"])
    finer = Mesh(mesh.devices.reshape(dims), AXES)
    split = P("gx", GY, "gz")
    return jax.shard_map(
        functools.partial(local, matchings(dims)),
        mesh=finer,
        in_specs=(split,) * 6,
        out_specs=(split, split),
        check_vma=False,
    )
```

```python
import functools

import jax
import jax.numpy as jnp
import numpy as np
from jax import lax
from jax.experimental import pallas as pl
from jax.experimental.pallas import tpu as pltpu
from jax.sharding import Mesh
from jax.sharding import PartitionSpec as P


AXES = ("gx", "gy_0", "gy_1", "gz")
GY = ("gy_0", "gy_1")
HIGHEST = lax.Precision.HIGHEST
LANES = 128
F32 = jnp.float32
BF16 = jnp.bfloat16


def involution(dims, partner):
    pairs = []
    for place in np.ndindex(*dims):
        pairs.append(
            (int(np.ravel_multi_index(place, dims)), int(np.ravel_multi_index(partner(*place), dims)))
        )
    back = dict(pairs)
    assert all(back[b] == a for a, b in pairs)
    return pairs


def shifted(i, n):
    return (i + 1) % n if i % 2 else (i - 1) % n


def matchings(dims):
    nx, ny, _, nz = dims

    def edge_core(x, y, c, z):
        return (x, y, 1 - c, z)

    def edge_x(x, y, c, z):
        return (x ^ 1, y, c, z)

    def second_y(x, y, c, z):
        other = y + 1 if c else y - 1
        return (x, other, 1 - c, z) if 0 <= other < ny else edge_x(x, y, c, z)

    return {
        "x1": involution(dims, edge_x),
        "z1": involution(dims, lambda x, y, c, z: (x, y, c, z ^ 1)),
        "x2": involution(
            dims, lambda x, y, c, z: (shifted(x, nx), y, c, z) if 0 < x < nx - 1 else edge_core(x, y, c, z)
        ),
        "z2": involution(
            dims, lambda x, y, c, z: (x, y, c, shifted(z, nz)) if 0 < z < nz - 1 else edge_core(x, y, c, z)
        ),
        "y2": involution(dims, second_y),
        "y1": involution(dims, edge_core),
        "ring": involution(dims, lambda x, y, c, z: (x, y, c, shifted(z, nz))),
        "far": involution(
            dims,
            lambda x, y, c, z: (x, y, c, (nz // 2 - 1 - z if z < nz // 2 else 3 * nz // 2 - 1 - z) if z % 4 in (0, 3) else nz - 1 - z),
        ),
    }


HALO = ("x1", "z1", "x2", "z2", "y2", "y1")
SLOTS = tuple((HALO.index(axis + "1"), HALO.index(axis + "2")) for axis in "xyz")


def swap(array, pairs):
    return lax.ppermute(array, AXES, pairs)


def of_everyone(array, axes):
    count = np.prod([lax.axis_size(axis) for axis in axes])
    return lax.all_to_all(jnp.broadcast_to(array, (count, *array.shape)), axes, 0, 0, tiled=True)


def places():
    x = lax.axis_index("gx")
    core = lax.axis_index("gy_1")
    y = lax.axis_index("gy_0") * 2 + core
    z = lax.axis_index("gz")
    return (
        (x, lax.axis_size("gx")),
        (y, lax.axis_size("gy_0") * lax.axis_size("gy_1")),
        (z, lax.axis_size("gz")),
    )


def permuter(maps_ref, d):
    width = maps_ref.shape[-1]
    rows = lax.broadcasted_iota(jnp.int32, (width, width), 0)
    return jnp.where(rows == maps_ref[d : d + 1, :], 1.0, 0.0).astype(BF16)


def in_three(values):
    first = values.astype(BF16)
    rest = values - first.astype(F32)
    second = rest.astype(BF16)
    third = (rest - second.astype(F32)).astype(BF16)
    return jnp.concatenate([first, second, third], axis=0)


def reordered(values, one_hot, back):
    rows = values.shape[0]
    dims = (((1,), (1,)), ((), ())) if back else (((1,), (0,)), ((), ()))
    parts = lax.dot_general(in_three(values), one_hot, dims, preferred_element_type=F32)
    return parts[:rows] + parts[rows : 2 * rows] + parts[2 * rows :]


def write_sends(vector_of, maps_ref, send_refs):
    for d, (position, _) in enumerate(places()):
        odd = lax.rem(position, 2) == 1
        minus = vector_of(2 * d)
        plus = vector_of(2 * d + 1)
        owner_minus = reordered(minus, permuter(maps_ref, d), True)
        first, second = SLOTS[d]
        send_refs[first][...] = jnp.where(odd, owner_minus, plus)
        send_refs[second][...] = jnp.where(odd, plus, owner_minus)


def difference(vector_ref, receive_refs, maps_ref):
    width = maps_ref.shape[-1]
    blocks = []
    for d, (position, extent) in enumerate(places()):
        odd = lax.rem(position, 2) == 1
        first, second = (receive_refs[slot][...] for slot in SLOTS[d])
        below = jnp.where(odd, first, second)
        above = jnp.where(odd, second, first)
        minus = vector_ref[:, 2 * d * width : (2 * d + 1) * width]
        plus = vector_ref[:, (2 * d + 1) * width : (2 * d + 2) * width]
        lower = minus - reordered(below, permuter(maps_ref, d), False)
        blocks.append(jnp.where(position > 0, lower, 0.0))
        blocks.append(jnp.where(position < extent - 1, plus - above, 0.0))
    return blocks


def times_operator(values, operator_ref):
    rows = values.shape[0]
    high = values.astype(BF16)
    low = (values - high.astype(F32)).astype(BF16)
    both = jnp.dot(
        jnp.concatenate([high, low], axis=0), operator_ref[...], preferred_element_type=F32
    )
    return both[:rows] + both[rows:]


def dot_rows(first, second):
    return lax.dot_general(
        first, second, (((1,), (1,)), ((), ())), precision=HIGHEST, preferred_element_type=F32
    )


def dot_columns(first, second):
    return lax.dot_general(
        first, second, (((0,), (0,)), ((), ())), precision=HIGHEST, preferred_element_type=F32
    )


def dot(first, second):
    return jnp.dot(first, second, precision=HIGHEST, preferred_element_type=F32)


def coarse(values, modes_ref, dual_modes_ref):
    return dot(dot_rows(values, dual_modes_ref[...]), modes_ref[...])


def blocks_of(array, width):
    return lambda i: array[:, i * width : (i + 1) * width]


def eliminate(matrix, others, count, block):
    rows = matrix.shape[0]
    row_number = lax.broadcasted_iota(jnp.int32, (rows, 1), 0)
    parts = [matrix, *others]
    for start in range(0, count, block):
        at = range(start, min(start + block, count))
        lines = [[part[k : k + 1, :] for part in parts] for k in at]
        entries = [[jnp.broadcast_to(line[0][:, j : j + 1], (1, LANES)) for j in at] for line in lines]
        for i in range(len(at)):
            inverse = 1.0 / entries[i][i]
            entries[i] = [entry * inverse for entry in entries[i]]
            lines[i] = [scaled(line, inverse) for line in lines[i]]
            for other in range(len(at)):
                if other != i:
                    factor = entries[other][i]
                    lines[other] = [
                        line - scaled(pivot, factor) for line, pivot in zip(lines[other], lines[i], strict=True)
                    ]
                    entries[other] = [
                        entry - factor * pivot for entry, pivot in zip(entries[other], entries[i], strict=True)
                    ]
        columns = [parts[0][:, k : k + 1] for k in at]
        for p in range(len(parts)):
            rest = parts[p]
            for column, line in zip(columns, lines, strict=True):
                rest = rest - column * line[p]
            for k, line in zip(at, lines, strict=True):
                rest = jnp.where(row_number == k, line[p], rest)
            parts[p] = rest
    return parts[1:]


def scaled(line, factor):
    size = line.shape[1]
    if size <= LANES:
        return line * factor[:, 0:size]
    return line * jnp.concatenate([factor] * (size // LANES), axis=1)


def start_kernel(
    counts_ref,
    modes_hbm,
    load_hbm,
    maps_hbm,
    operator_hbm,
    dual_load_hbm,
    modes_ref,
    dual_ref,
    vector_ref,
    maps_ref,
    operator_ref,
    dual_load_ref,
    *refs,
):
    send_refs, (modes_in_ref, load_ref, sems) = refs[:-3], refs[-3:]
    copies = [
        pltpu.make_async_copy(source, target, sems.at[i])
        for i, (source, target) in enumerate(
            (
                (modes_hbm, modes_in_ref),
                (load_hbm, load_ref),
                (maps_hbm, maps_ref),
                (operator_hbm, operator_ref),
                (dual_load_hbm, dual_load_ref),
            )
        )
    ]
    for copy in copies:
        copy.start()
    for copy in copies[:3]:
        copy.wait()
    width = maps_ref.shape[-1]
    count = counts_ref[0]
    total, size = modes_in_ref.shape
    rows = modes_ref.shape[0]
    modes_ref[...] = jnp.zeros_like(modes_ref)
    lane = lax.broadcasted_iota(jnp.int32, (total, width), 0)
    for d, (position, extent) in enumerate(places()):
        for side, there in ((0, position > 0), (1, position < extent - 1)):
            part = pl.ds((2 * d + side) * width, width)
            keep = jnp.logical_and(lane < count, there)
            modes_ref[0:total, part] = jnp.where(keep, modes_in_ref[:, part], 0.0)
    modes = modes_ref[...]
    one = lax.broadcasted_iota(jnp.int32, (rows, rows), 0)
    two = lax.broadcasted_iota(jnp.int32, (rows, rows), 1)
    normal = dot_rows(modes, modes) + jnp.where(jnp.logical_and(one == two, one >= count), 1.0, 0.0)
    row = lax.broadcasted_iota(jnp.int32, load_ref.shape, 0)
    dual_ref[...] = jnp.zeros_like(dual_ref)
    dual_ref[0:total, 0 : load_ref.shape[1]] = jnp.where(row < count, load_ref[...], 0.0)
    loads = dual_ref[:, 0 : load_ref.shape[1]]
    dual, coefficients = eliminate(normal, [modes, loads], total, 2)
    dual_ref[...] = dual
    vector = dot_columns(coefficients, modes)
    vector_ref[...] = vector
    write_sends(blocks_of(vector, width), maps_ref, send_refs)
    for copy in copies[3:]:
        copy.wait()


def first_kernel(operator_ref, load_ref, vector_ref, maps_ref, *refs):
    receive_refs, (lambda_ref, next_ref), send_refs = refs[:6], refs[6:8], refs[8:]
    width = maps_ref.shape[-1]
    blocks = difference(vector_ref, receive_refs, maps_ref)
    for d in range(3):
        lambda_ref[:, d * width : (d + 1) * width] = blocks[2 * d + 1]
    product = times_operator(jnp.concatenate(blocks, axis=1), operator_ref)
    parts = []
    for i in range(6):
        part = product[:, i * width : (i + 1) * width]
        parts.append(load_ref[:, (i // 2) * width : (i // 2 + 1) * width] - part if i % 2 else -part)
        next_ref[:, i * width : (i + 1) * width] = parts[i]
    write_sends(lambda i: parts[i], maps_ref, send_refs)


def coarse_kernel(modes_ref, dual_ref, vector_ref, maps_ref, *refs):
    receive_refs, (whole_ref, next_ref), send_refs = refs[:6], refs[6:8], refs[8:]
    width = maps_ref.shape[-1]
    whole = jnp.concatenate(difference(vector_ref, receive_refs, maps_ref), axis=1)
    whole_ref[...] = whole
    following = coarse(whole, modes_ref, dual_ref)
    next_ref[...] = following
    write_sends(blocks_of(following, width), maps_ref, send_refs)


def operator_kernel(operator_ref, base_ref, before_ref, vector_ref, maps_ref, *refs):
    receive_refs, (whole_ref, next_ref, gram_ref), send_refs = refs[:6], refs[6:9], refs[9:]
    width = maps_ref.shape[-1]
    whole = base_ref[...] - 0.25 * jnp.concatenate(
        difference(vector_ref, receive_refs, maps_ref), axis=1
    )
    whole_ref[...] = whole
    product = times_operator(whole, operator_ref)
    next_ref[...] = product
    write_sends(blocks_of(product, width), maps_ref, send_refs)
    gram_ref[...] = dot_rows(whole, jnp.concatenate([before_ref[...], product], axis=0))


def last_kernel(operator_ref, base_ref, before_ref, vector_ref, gram_in_ref, maps_ref, *refs):
    receive_refs, (whole_ref, next_ref, gram_ref), send_refs = refs[:6], refs[6:9], refs[9:]
    width = maps_ref.shape[-1]
    whole = base_ref[...] - 0.25 * jnp.concatenate(
        difference(vector_ref, receive_refs, maps_ref), axis=1
    )
    whole_ref[...] = whole
    product = times_operator(whole, operator_ref)
    next_ref[...] = product
    half = gram_in_ref.shape[1]
    gram_ref[:, 0:half] = gram_in_ref[...]
    gram_ref[:, half:] = dot_rows(whole, jnp.concatenate([before_ref[...], product], axis=0))
    for d in range(3):
        minus = product[:, 2 * d * width : (2 * d + 1) * width]
        send_refs[d][...] = reordered(minus, permuter(maps_ref, d), True)


def finish_kernel(
    gram_ref, lambda_ref, first_ref, second_ref, residual_ref, image_ref, product_ref, *refs
):
    receive_refs, (multipliers_ref, out_ref) = refs[:6], refs[6:]
    count = gram_ref.shape[0]
    width = product_ref.shape[1] // 6
    total = gram_ref[...]
    right = total[:, 0:count]
    energy, cross, last = (total[:, i * count : (i + 1) * count] for i in (1, 2, 3))
    energy = 0.5 * (energy + energy.T)
    last = 0.5 * (last + last.T)
    upper = jnp.concatenate([energy, cross.T, right], axis=1)
    lower = jnp.concatenate([cross, last, energy], axis=1)
    rows = 2 * count
    (solved,) = eliminate_whole(jnp.concatenate([upper, lower], axis=0), rows)
    steps = solved.T
    for d, (position, extent) in enumerate(places()):
        odd = lax.rem(position, 2) == 1
        first, second = (receive_refs[slot][...] for slot in SLOTS[d])
        above = jnp.where(odd, second, first)
        at = slice((2 * d + 1) * width, (2 * d + 2) * width)
        to = slice(d * width, (d + 1) * width)
        second_image = jnp.where(position < extent - 1, product_ref[:, at] - above, 0.0)
        directions = jnp.concatenate([first_ref[:, at], second_ref[:, at]], axis=0)
        images = jnp.concatenate([image_ref[:, at], second_image], axis=0)
        multipliers_ref[:, to] = lambda_ref[:, to] + dot(steps, directions)
        out_ref[:, to] = residual_ref[:, at] - dot(steps, images)


def eliminate_whole(matrix, count):
    block = 4
    row_number = lax.broadcasted_iota(jnp.int32, (matrix.shape[0], 1), 0)
    size = matrix.shape[1]
    for start in range(0, count, block):
        lines = [matrix[start + i : start + i + 1, :] for i in range(block)]
        entries = [
            [jnp.broadcast_to(line[:, start + j : start + j + 1], (1, size)) for j in range(block)]
            for line in lines
        ]
        for i in range(block):
            inverse = 1.0 / entries[i][i]
            entries[i] = [entry * inverse for entry in entries[i]]
            lines[i] = lines[i] * inverse
            for other in range(block):
                if other != i:
                    factor = entries[other][i]
                    lines[other] = lines[other] - factor * lines[i]
                    entries[other] = [e - factor * p for e, p in zip(entries[other], entries[i], strict=True)]
        rest = matrix
        for i in range(block):
            rest = rest - matrix[:, start + i : start + i + 1] * lines[i]
        for i in range(block):
            rest = jnp.where(row_number == start + i, lines[i], rest)
        matrix = rest
    return (matrix[:, count:],)


def call(kernel, outs, *operands, spaces=(), scratch=()):
    specs = [
        pl.BlockSpec(memory_space=spaces[i] if i < len(spaces) else pltpu.VMEM) for i in range(len(operands))
    ]
    return pl.pallas_call(
        kernel,
        out_shape=[o if isinstance(o, jax.ShapeDtypeStruct) else jax.ShapeDtypeStruct(o, F32) for o in outs],
        in_specs=specs,
        out_specs=[pl.BlockSpec(memory_space=pltpu.VMEM)] * len(outs),
        scratch_shapes=scratch,
        compiler_params=pltpu.CompilerParams(vmem_limit_bytes=16 * 2**20),
        name=kernel.__name__,
    )(*operands)


def local(pairs, dual_operators, dual_load, rigid_modes, coarse_load, mode_counts, face_maps):
    operator = dual_operators[0, 0, 0]
    load = dual_load[0, 0, 0]
    modes_in = rigid_modes[0, 0, 0]
    coefficients = coarse_load[0, 0, 0]
    counts = mode_counts.reshape(1)
    maps = face_maps[0, 0, 0]
    cases = load.shape[0]
    size = operator.shape[0]
    width = maps.shape[1]
    full, face = (cases, size), (cases, width)
    padded = (-(-modes_in.shape[0] // 8) * 8, size)

    def halo(sends):
        return [swap(send, pairs[name]) for send, name in zip(sends, HALO, strict=True)]

    modes, dual, vector, maps, operator, load, *sends = call(
        start_kernel,
        [
            padded,
            padded,
            full,
            jax.ShapeDtypeStruct(maps.shape, maps.dtype),
            jax.ShapeDtypeStruct(operator.shape, operator.dtype),
            load.shape,
            *[face] * 6,
        ],
        counts,
        modes_in,
        coefficients,
        maps,
        operator,
        load,
        spaces=(pltpu.SMEM, *[pltpu.HBM] * 5),
        scratch=[
            pltpu.VMEM(modes_in.shape, F32),
            pltpu.VMEM(coefficients.shape, F32),
            pltpu.SemaphoreType.DMA((5,)),
        ],
    )
    initial, load_vector, *sends = call(
        first_kernel, [load.shape, full, *[face] * 6], operator, load, vector, maps, *halo(sends)
    )
    residual, vector, *sends = call(
        coarse_kernel, [full, full, *[face] * 6], modes, dual, load_vector, maps, *halo(sends)
    )
    first, product, gram, *sends = call(
        operator_kernel,
        [full, full, (cases, 2 * cases), *[face] * 6],
        operator,
        residual,
        load_vector,
        vector,
        maps,
        *halo(sends),
    )
    image, vector, *sends = call(
        coarse_kernel, [full, full, *[face] * 6], modes, dual, product, maps, *halo(sends)
    )
    second, product, gram, *sends = call(
        last_kernel,
        [full, full, (cases, 4 * cases), *[face] * 3],
        operator,
        image,
        product,
        vector,
        gram,
        maps,
        *halo(sends),
    )
    gram = gram + swap(gram, pairs["y1"])
    gram = of_everyone(gram, ("gx", "gy_0")).sum(axis=0)
    gram, *sends = lax.optimization_barrier((gram, *sends))
    gram = gram + swap(gram, pairs["z1"])
    gram = gram + swap(gram, pairs["ring"])
    gram = gram + swap(gram, pairs["far"])
    multipliers, out = call(
        finish_kernel,
        [load.shape, load.shape],
        gram,
        initial,
        first,
        second,
        residual,
        image,
        product,
        *halo([sends["xyz".index(name[0])] for name in HALO]),
    )
    return multipliers[None, None, None], out[None, None, None]


def solution(mesh):
    dims = (mesh.shape["gx"], mesh.shape["gy"] // 2, 2, mesh.shape["gz"])
    finer = Mesh(mesh.devices.reshape(dims), AXES)
    split = P("gx", GY, "gz")
    return jax.shard_map(
        functools.partial(local, matchings(dims)),
        mesh=finer,
        in_specs=(split,) * 6,
        out_specs=(split, split),
        check_vma=False,
    )
```
